32 devices in a mesh: val: 8 (over y, x, core), cond: 4 (over z).
Axes of the slice: x: 2, y: 2, z: 4, core: 2. Of those that a mesh axis runs over, the one named last changes fastest.
Arguments:
- trial: bfloat16 [256, 65536], P('val', 'cond'), may hold values from -6 to 6
- pair_cond: bfloat16 [80, 1024, 1024], P('val', 'cond'), may hold values from -0.1875 to 0.1875
- pair_val: bfloat16 [256, 20480], P(None, 'val'), may hold values from -0.0625 to 0.0625
Outputs:
- applied: bfloat16 [256, 65536], P('val', 'cond')
The draws below stay inside these ranges and needn't reach their ends.
All inputs are finite; a program needn't handle non-finite values.
Results may differ from the reference program's by a relative error of at most 0.0049.
Values may be sent and summed in bfloat16 or wider, within the bound.
No kernel may reach another device: no remote copies, remote signals or barrier semaphores. Data moves between devices by JAX's collectives and lax.ppermute only.
A program may use at most 320 MiB of HBM per device.

```python
import jax
import jax.numpy as jnp
from jax import lax

V = 256
C = 1024
S = 64
G = 80


def with_spikes(values, rng, source, target, parts, factor):
    def block_of(dim):
        return (jnp.arange(values.shape[dim]) // (values.shape[dim] // parts)).reshape((-1,) + (1,) * (values.ndim - 1 - dim))

    first = jax.random.permutation(rng, parts)[block_of(target)]
    other_side = (block_of(target) + parts // 2) % parts
    return jnp.where((block_of(source) == first) | (block_of(source) == other_side), factor * values, values)


def shard_levels(own_key, extent, pieces, low, largest):
    def one(dim, blocks):
        draws = jax.random.uniform(jax.random.fold_in(jax.random.fold_in(own_key, 6), dim), (blocks,), jnp.float32, low / len(pieces), largest / len(pieces))
        return jnp.repeat(jnp.exp(draws), extent[dim] // blocks).reshape((-1,) + (1,) * (len(extent) - dim - 1))

    factor_of = one(*pieces[0])
    for cut in pieces[1:]:
        factor_of = factor_of * one(*cut)
    return factor_of


def normal_values(key, shape, scale, limit, cuts=(), kind=jnp.bfloat16):
    loudness = shard_levels(key, shape, cuts, -0.22, 0.18) if cuts else 1.0
    values = jax.random.normal(key, shape, jnp.float32) * scale * loudness
    return jnp.minimum(jnp.maximum(values, -limit), limit).astype(kind)


def noise_with(key, extent, width, most, split, heavy, kind=jnp.bfloat16):
    values = width * jax.random.normal(key, extent, jnp.float32)
    if split:
        values = values * shard_levels(key, extent, split, -0.22, 0.18)
    return jnp.clip(with_spikes(values, jax.random.fold_in(key, 3), *heavy), -most, most).astype(kind)


def setup_inputs(seed: int = 0) -> dict:
    streams_of = jax.random.split(jax.random.key(seed), 4)
    return {
        "trial": normal_values(streams_of[0], (V, C * S), 1.0, 6.0, ((0, 8), (1, 4))),
        "pair_cond": normal_values(streams_of[1], (G, C, C), C ** -0.5, 0.1875, ((0, 8), (1, 4))),
        "pair_val": noise_with(streams_of[2], (V, V * G), (V * G) ** -0.5, 0.0625, ((1, 8),), (1, 0, 8, 2.0)),
    }


def reference(trial, pair_cond, pair_val):
    trial_wide = trial.astype(jnp.float32).reshape(V, C, S)
    val_wide = pair_val.reshape(V, V, G)

    def advance(total, index):
        cond_slab = lax.dynamic_index_in_dim(pair_cond, index, 0, keepdims=False).astype(jnp.float32)
        val_slab = lax.dynamic_index_in_dim(val_wide, index, 2, keepdims=False).astype(jnp.float32)
        inner = jnp.einsum("cd,wds->wcs", cond_slab, trial_wide).astype(jnp.bfloat16)
        total = total + jnp.einsum("vw,wcs->vcs", val_slab, inner.astype(jnp.float32))
        return total, None

    start = jnp.zeros((V, C, S), jnp.float32)
    total, _ = lax.scan(advance, start, jnp.arange(G, dtype=jnp.int32))
    return total.reshape(V, C * S).astype(jnp.bfloat16)
```

```python
import jax
import jax.numpy as jnp
from jax import lax
from jax.experimental import pallas as pl
from jax.experimental.pallas import tpu as pltpu
from jax.sharding import PartitionSpec as P

S = 64
G = 80
CHUNKS = 4

NT = (((1,), (1,)), ((), ()))
NN = (((1,), (0,)), ((), ()))


def group_size(count, rows):
    best = 1
    for size in range(1, count + 1):
        if count % size == 0 and size * rows <= 256:
            best = size
    return best


def chain(zed, units, pc, pv_units, acc):
    pieces = len(units[0])
    count, rows, depth = units[0][0].shape
    total_g, cols, _ = pc.shape
    bands = pv_units[0].shape[2]
    many = len(units)
    gg = group_size(total_g, rows * many)
    high = gg * many * rows
    first = acc is None

    def kernel(zed_ref, *refs):
        refs = list(refs)
        t_refs = [[refs.pop(0) for _ in range(pieces)] for _ in range(many)]
        pc_refs = [refs.pop(0) for _ in range(pieces)]
        pv_refs = [refs.pop(0) for _ in range(many)]
        acc_ref = None if first else refs.pop(0)
        out_ref, inner_ref = refs

        @pl.when(pl.program_id(0) == 0)
        def _():
            if first:
                out_ref[...] = jnp.zeros(out_ref.shape, jnp.float32)
            else:
                out_ref[...] = acc_ref[...]

        stacked = jnp.concatenate([pv_refs[u][g] for g in range(gg) for u in range(many)], axis=0)
        left = stacked.T
        for g in range(gg):
            for u in range(many):
                low = (g * many + u) * rows
                inner = None
                for q in range(pieces):
                    part = lax.dot_general(
                        t_refs[u][q][...].reshape(count * rows, depth), pc_refs[q][g], NT,
                        preferred_element_type=jnp.float32)
                    inner = part if inner is None else inner + part
                inner_ref[:, low:low + rows, :] = inner.astype(jnp.bfloat16).reshape(count, rows, cols)
        for s in range(count):
            out_ref[s] += lax.dot_general(left, inner_ref[s], NN, preferred_element_type=jnp.float32)

    def fixed(i, z):
        return (0, 0, 0)

    def piece_map(q):
        return lambda i, z: (i, 0, lax.rem(z[0] + (pieces - q), pieces))

    def tall_map(q):
        return lambda i, z: (lax.rem(z[0] + (pieces - q), pieces), i, 0, 0)

    in_specs = [pl.BlockSpec((count, rows, depth), fixed) for _ in range(many * pieces)]
    if depth % 128:
        pc = pc.reshape(total_g, cols, pieces, depth).transpose(2, 0, 1, 3)
        in_specs += [pl.BlockSpec((None, gg, cols, depth), tall_map(q)) for q in range(pieces)]
    else:
        in_specs += [pl.BlockSpec((gg, cols, depth), piece_map(q)) for q in range(pieces)]
    in_specs += [pl.BlockSpec((gg, rows, bands), lambda i, z: (i, 0, 0)) for _ in range(many)]
    operands = [p for unit in units for p in unit] + [pc] * pieces + list(pv_units)
    aliases = {}
    if not first:
        in_specs.append(pl.BlockSpec((count, bands, cols), fixed))
        operands.append(acc)
        aliases = {len(operands): 0}
    flops = 2 * count * total_g * many * rows * cols * (pieces * depth + bands)
    return pl.pallas_call(
        kernel,
        out_shape=jax.ShapeDtypeStruct((count, bands, cols), jnp.float32),
        grid_spec=pltpu.PrefetchScalarGridSpec(
            num_scalar_prefetch=1,
            grid=(total_g // gg,),
            in_specs=in_specs,
            out_specs=pl.BlockSpec((count, bands, cols), fixed),
            scratch_shapes=[pltpu.VMEM((count, high, cols), jnp.bfloat16)],
        ),
        input_output_aliases=aliases,
        compiler_params=pltpu.CompilerParams(
            dimension_semantics=("arbitrary",), vmem_limit_bytes=48 * 1024 * 1024),
        cost_estimate=pl.CostEstimate(
            flops=flops, transcendentals=0,
            bytes_accessed=total_g * cols * depth * pieces * 2 + count * bands * cols * 8),
        name="chain",
    )(zed, *operands)


def make_body(mesh):
    nv, nc = mesh.shape["val"], mesh.shape["cond"]
    nx = nv // 4

    def split(i):
        return i // (2 * nx), (i // 2) % nx, i % 2

    def join(y, x, k):
        return (y * nx + x) * 2 + k

    def twin_of(i):
        return i ^ 1

    def flip_y(i):
        return lax.rem(i + 2 * nx, nv) if not isinstance(i, int) else (i + 2 * nx) % nv

    def send(value, table):
        return lax.ppermute(value, "val", table)

    to_twin = [(i, i ^ 1) for i in range(nv)]
    to_y = [(i, (i + 2 * nx) % nv) for i in range(nv)]

    def to_x(step):
        return [(i, join(split(i)[0], (split(i)[1] + step) % nx, split(i)[2])) for i in range(nv)]

    def to_z(step):
        return [(j, (j + step) % nc) for j in range(nc)]

    def body(trial, pair_cond, pair_val):
        me = lax.axis_index("val")
        zed = lax.axis_index("cond").astype(jnp.int32).reshape(1)
        core = lax.rem(me, 2)
        own_x = lax.rem(me // 2, nx)
        own_y = me // (2 * nx)
        wb = trial.shape[0]
        depth = trial.shape[1] // S
        bands = pair_val.shape[0]
        gb, cols, _ = pair_cond.shape
        vb = bands // nv
        half = S // 2
        n = half // CHUNKS

        turned = trial.reshape(wb, depth, S).transpose(2, 0, 1)
        kept = lax.dynamic_slice_in_dim(turned, core * half, half, 0)
        given = lax.dynamic_slice_in_dim(turned, (1 - core) * half, half, 0)
        block = jnp.concatenate([kept, send(given, to_twin)], axis=1)

        flat = pair_val.T.reshape(wb, nv, gb, bands).transpose(1, 2, 0, 3)

        def blocks_for(dest):
            order = (dest, dest ^ 1, flip_y(dest), flip_y(dest) ^ 1)
            return jnp.stack([lax.dynamic_index_in_dim(flat, o, 0, keepdims=False) for o in order])

        def swap_pairs(a):
            return jnp.stack([a[1], a[0], a[3], a[2]])

        pv_units = [jnp.concatenate([blocks_for(me), send(blocks_for(me ^ 1), to_twin)], axis=2)]
        for step in range(1, nx):
            dest = (own_y * nx + lax.rem(own_x + step, nx)) * 2 + core
            got = send(blocks_for(dest), to_x(step))
            pv_units.append(jnp.concatenate([got, send(swap_pairs(got), to_twin)], axis=2))
        pv_own = [u[:2].reshape(2 * gb, 2 * wb, bands) for u in pv_units]

        pc_own = jnp.concatenate([pair_cond, send(pair_cond, to_twin)], axis=0)
        cut = (gb * 2) // 5
        far = []
        for lo, hi in ((0, cut), (cut, gb)):
            got = send(pair_cond[lo:hi], to_y)
            pcs = jnp.concatenate([got, send(got, to_twin)], axis=0)
            pvs = [u[2:, lo:hi].reshape(2 * (hi - lo), 2 * wb, bands) for u in pv_units]
            far.append((pcs, pvs))

        units = []
        for i in range(CHUNKS):
            part = block[i * n:(i + 1) * n]
            near = [part] + [lax.ppermute(part, "cond", to_z(q)) for q in range(1, nc)]
            units.append([near])
        for i in range(CHUNKS):
            near = units[i][0]
            for step in range(1, nx):
                units[i].append([send(p, to_x(step)) for p in near])

        accs = []
        for i in range(CHUNKS):
            acc = chain(zed, units[i][:1], pc_own, pv_own[:1], None)
            accs.append(acc)
        for i in range(CHUNKS):
            for u in range(1, nx):
                accs[i] = chain(zed, units[i][u:u + 1], pc_own, pv_own[u:u + 1], accs[i])
            pcs, pvs = far[0]
            for u in range(0, nx, 2):
                accs[i] = chain(zed, units[i][u:u + 2], pcs, pvs[u:u + 2], accs[i])
        finals = []
        for i in range(CHUNKS):
            pcs, pvs = far[1]
            for u in range(0, nx, 2):
                accs[i] = chain(zed, units[i][u:u + 2], pcs, pvs[u:u + 2], accs[i])
            shaped = accs[i].reshape(n, 2, nx, 2 * vb, cols)
            total = lax.dynamic_index_in_dim(shaped, own_x, 2, keepdims=False)
            for step in range(1, nx):
                other = lax.dynamic_index_in_dim(shaped, lax.rem(own_x + step, nx), 2, keepdims=False)
                total = total + send(other.astype(jnp.bfloat16), to_x(step)).astype(jnp.float32)
            other = lax.dynamic_index_in_dim(total, 1 - own_y, 1, keepdims=False)
            mine = lax.dynamic_index_in_dim(total, own_y, 1, keepdims=False)
            mine = mine + send(other.astype(jnp.bfloat16), to_y).astype(jnp.float32)
            finals.append(mine.astype(jnp.bfloat16))
        done = jnp.concatenate(finals, axis=0).reshape(half, 2, vb, cols)
        mine = lax.dynamic_index_in_dim(done, core, 1, keepdims=False)
        other = send(lax.dynamic_index_in_dim(done, 1 - core, 1, keepdims=False), to_twin)
        low = jnp.where(core == 0, mine, other)
        high = jnp.where(core == 0, other, mine)
        whole = jnp.concatenate([low, high], axis=0)
        return whole.transpose(1, 2, 0).reshape(vb, cols * S)

    return body


def solution(mesh):
    placed = (P("val", "cond"), P("val", "cond", None), P(None, "val"))
    return jax.shard_map(
        make_body(mesh), mesh=mesh, in_specs=placed, out_specs=P("val", "cond"), check_vma=False
    )
```

```python
import jax
import jax.numpy as jnp
from jax import lax
from jax.experimental import pallas as pl
from jax.experimental.pallas import tpu as pltpu
from jax.sharding import PartitionSpec as P


S = 64
CHUNKS = 4
GROUPS = 1

NT = (((1,), (1,)), ((), ()))
NN = (((1,), (0,)), ((), ()))


def group_size(count, rows):
    best = 1
    for size in range(1, count + 1):
        if count % size == 0 and size * rows <= 256:
            best = size
    return best


def chain(zed, entries, pc, accs):
    pieces, count, rows, depth = entries[0][0][0].shape
    total_g, cols, _ = pc.shape
    bands = entries[0][0][1].shape[2]
    many = len(entries[0])
    gg = group_size(total_g, rows * many)
    step_g = gg * GROUPS if total_g % (gg * GROUPS) == 0 else gg
    high = gg * many * rows
    first = [acc is None for acc in accs]

    def kernel(zed_ref, *refs):
        refs = list(refs)
        pc_ref = refs.pop(0)
        zed_at = zed_ref[0]
        t_refs = [[refs.pop(0) for _ in entry] for entry in entries]
        pv_refs = [[refs.pop(0) for _ in entry] for entry in entries]
        acc_refs = [None if f else refs.pop(0) for f in first]
        out_refs = [refs.pop(0) for _ in entries]
        token_ref, inner_ref = refs

        @pl.when(pl.program_id(0) == 0)
        def _():
            token_ref[...] = jnp.zeros(token_ref.shape, jnp.float32)
            for acc_ref, out_ref in zip(acc_refs, out_refs):
                if acc_ref is None:
                    out_ref[...] = jnp.zeros(out_ref.shape, jnp.float32)
                else:
                    out_ref[...] = acc_ref[...]

        for e in range(len(entries)):
            for base in range(0, step_g, gg):
                stacked = jnp.concatenate(
                    [pv_refs[e][u][base + g] for g in range(gg) for u in range(many)], axis=0)
                left = stacked.T
                for g in range(gg):
                    for u in range(many):
                        low = (g * many + u) * rows
                        inner = None
                        for d in range(pieces):
                            q = lax.rem(zed_at + (pieces - d), pieces)
                            if depth % 128:
                                weights = pc_ref[d, base + g]
                            else:
                                weights = pc_ref[base + g, :, d * depth:(d + 1) * depth]
                            part = lax.dot_general(
                                t_refs[e][u][q].reshape(count * rows, depth), weights, NT,
                                preferred_element_type=jnp.float32)
                            inner = part if inner is None else inner + part
                        inner_ref[e, :, low:low + rows, :] = inner.astype(jnp.bfloat16).reshape(count, rows, cols)
                for s in range(count):
                    out_refs[e][s] += lax.dot_general(left, inner_ref[e, s], NN, preferred_element_type=jnp.float32)

    def fixed(i, z):
        return (0, 0, 0)

    if depth % 128:
        pc = pc.reshape(total_g, cols, pieces, depth).transpose(2, 0, 1, 3)
        in_specs = [pl.BlockSpec((pieces, step_g, cols, depth), lambda i, z: (0, i, 0, 0))]
    else:
        in_specs = [pl.BlockSpec((step_g, cols, pieces * depth), lambda i, z: (i, 0, 0))]
    flat = [unit for entry in entries for unit in entry]
    in_specs += [pl.BlockSpec((pieces, count, rows, depth), lambda i, z: (0, 0, 0, 0)) for _ in flat]
    in_specs += [pl.BlockSpec((step_g, rows, bands), lambda i, z: (i, 0, 0)) for _ in flat]
    operands = [pc] + [t for t, _ in flat] + [pv for _, pv in flat]
    aliases = {}
    for e, acc in enumerate(accs):
        if acc is not None:
            in_specs.append(pl.BlockSpec((count, bands, cols), fixed))
            operands.append(acc)
            aliases[len(operands)] = e
    flops = 2 * len(flat) * count * total_g * rows * cols * (pieces * depth + bands)
    *outs, token = pl.pallas_call(
        kernel,
        out_shape=[jax.ShapeDtypeStruct((count, bands, cols), jnp.float32) for _ in entries]
        + [jax.ShapeDtypeStruct((8, 128), jnp.float32)],
        grid_spec=pltpu.PrefetchScalarGridSpec(
            num_scalar_prefetch=1,
            grid=(total_g // step_g,),
            in_specs=in_specs,
            out_specs=[pl.BlockSpec((count, bands, cols), fixed) for _ in entries]
            + [pl.BlockSpec((8, 128), lambda i, z: (0, 0))],
            scratch_shapes=[pltpu.VMEM((len(entries), count, high, cols), jnp.bfloat16)],
        ),
        input_output_aliases=aliases,
        compiler_params=pltpu.CompilerParams(
            dimension_semantics=("arbitrary",), vmem_limit_bytes=56 * 1024 * 1024),
        cost_estimate=pl.CostEstimate(
            flops=flops, transcendentals=0,
            bytes_accessed=total_g * cols * depth * pieces * 2 + len(entries) * count * bands * cols * 8),
        name="chain",
    )(zed, *operands)
    return outs, token


def after(value, *tokens):
    return lax.optimization_barrier((value, *tokens))[0]


def make_body(mesh):
    nv, nc = mesh.shape["val"], mesh.shape["cond"]
    nx = nv // 4

    def split(i):
        return i // (2 * nx), (i // 2) % nx, i % 2

    def join(y, x, k):
        return (y * nx + x) * 2 + k

    def flip_y(i):
        return lax.rem(i + 2 * nx, nv) if not isinstance(i, int) else (i + 2 * nx) % nv

    def send(value, table):
        return lax.ppermute(value, "val", table)

    to_twin = [(i, i ^ 1) for i in range(nv)]
    to_y = [(i, (i + 2 * nx) % nv) for i in range(nv)]

    def to_x(step):
        return [(i, join(split(i)[0], (split(i)[1] + step) % nx, split(i)[2])) for i in range(nv)]

    def to_z(step):
        return [(j, (j + step) % nc) for j in range(nc)]

    def body(trial, pair_cond, pair_val):
        me = lax.axis_index("val")
        zed = lax.axis_index("cond").astype(jnp.int32).reshape(1)
        core = lax.rem(me, 2)
        own_x = lax.rem(me // 2, nx)
        own_y = me // (2 * nx)
        wb = trial.shape[0]
        depth = trial.shape[1] // S
        bands = pair_val.shape[0]
        gb, cols, _ = pair_cond.shape
        vb = bands // nv
        half = S // 2
        n = half // CHUNKS

        pc_y = send(pair_cond, to_y)

        turned = trial.reshape(wb, depth, S).transpose(2, 0, 1)
        kept = lax.dynamic_slice_in_dim(turned, core * half, half, 0)
        given = lax.dynamic_slice_in_dim(turned, (1 - core) * half, half, 0)
        taken = send(given, to_twin)
        block = jnp.concatenate([kept, taken], axis=1)

        def around_z(part):
            return [part] + [lax.ppermute(part, "cond", to_z(q)) for q in range(1, nc)]

        parts = [around_z(block[:n])]

        flat = after(pair_val, block).T.reshape(wb, nv, gb, bands).transpose(1, 2, 0, 3)

        def blocks_for(dest):
            order = (dest, dest ^ 1, flip_y(dest), flip_y(dest) ^ 1)
            return jnp.stack([lax.dynamic_index_in_dim(flat, o, 0, keepdims=False) for o in order])

        def swap_pairs(a):
            return jnp.stack([a[1], a[0], a[3], a[2]])

        mine, twins = blocks_for(me), blocks_for(me ^ 1)
        far = []
        for step in range(1, nx):
            dest = (own_y * nx + lax.rem(own_x + step, nx)) * 2 + core
            far.append(blocks_for(dest))
        pv_near = jnp.concatenate([mine, send(twins, to_twin)], axis=2)
        far_got = [send(f, to_x(step)) for f, step in zip(far, range(1, nx))]
        pc_own = jnp.concatenate([pair_cond, send(after(pair_cond, block), to_twin)], axis=0)
        for i in range(1, CHUNKS):
            parts.append(around_z(after(block[i * n:(i + 1) * n], *far)))

        def own_pv(pv):
            return pv[:2].reshape(2 * gb, 2 * wb, bands)

        accs = [None] * CHUNKS
        near, others = [None] * CHUNKS, [None] * CHUNKS
        token = None
        pv_all = [pv_near]
        for i in range(CHUNKS):
            got = list(lax.optimization_barrier((*parts[i], pc_own if token is None else token))[:-1])
            near[i] = jnp.stack(got)
            others[i] = [send(near[i], to_x(step)) for step in range(1, nx)]
            work = [(i, [(near[i], own_pv(pv_near))])]
            if i:
                for u in range(1, nx):
                    other = after(others[i - 1][u - 1], token)
                    work.append((i - 1, [(other, own_pv(pv_all[u]))]))
            for w in (work if nx > 2 else [work]):
                w = w if isinstance(w, list) else [w]
                outs, token = chain(zed, [e for _, e in w], pc_own, [accs[j] for j, _ in w])
                for (j, _), out in zip(w, outs):
                    accs[j] = out
            if i == 0:
                for got in far_got:
                    got = after(got, token)
                    pv_all.append(jnp.concatenate([got, send(swap_pairs(got), to_twin)], axis=2))
        pc_y = after(pc_y, token)
        pc_yt = send(pc_y, to_twin)

        def both(i, u, which):
            return [(t, pv[2 + which]) for t, pv in list(zip([near[i]] + others[i], pv_all))[u:u + 2]]

        def far_call(chunks, which, pc, token):
            for u in range(0, nx, 2):
                outs, token = chain(
                    zed, [both(i, u, which) for i in chunks], after(pc, token), [accs[i] for i in chunks])
                for i, out in zip(chunks, outs):
                    accs[i] = out
            return token

        last = CHUNKS - 1
        token = far_call([0, 1], 0, pc_y, token)
        for u in range(1, nx):
            (accs[last],), token = chain(
                zed, [[(after(others[last][u - 1], token), own_pv(pv_all[u]))]], pc_own, [accs[last]])
        token = far_call([2, 3], 0, pc_y, token)

        def reduced(i):
            shaped = accs[i].reshape(n, 2, nx, 2 * vb, cols)

            def rows_of(y, x):
                block = lax.dynamic_slice(shaped, (0, y, x, 0, 0), (n, 1, 1, 2 * vb, cols))
                return block.reshape(n, 2 * vb, cols)

            total = rows_of(own_y, own_x)
            for dy in range(2):
                for dx in range(nx):
                    if dy or dx:
                        x = lax.rem(own_x + dx, nx)
                        y = own_y if dy == 0 else 1 - own_y
                        table = [
                            (j, join((split(j)[0] + dy) % 2, (split(j)[1] + dx) % nx, split(j)[2])) for j in range(nv)]
                        total = total + send(rows_of(y, x).astype(jnp.bfloat16), table).astype(jnp.float32)
            return total.astype(jnp.bfloat16)

        finals = []
        for chunks in ([0, 1], [2], [3]):
            token = far_call(chunks, 1, pc_yt, token)
            finals += [reduced(i) for i in chunks]
        done = jnp.concatenate(finals, axis=0).reshape(half, 2, vb, cols)
        mine = lax.dynamic_index_in_dim(done, core, 1, keepdims=False)
        other = send(lax.dynamic_index_in_dim(done, 1 - core, 1, keepdims=False), to_twin)
        low = jnp.where(core == 0, mine, other)
        high = jnp.where(core == 0, other, mine)
        whole = jnp.concatenate([low, high], axis=0)
        return whole.transpose(1, 2, 0).reshape(vb, cols * S)

    return body


def solution(mesh):
    placed = (P("val", "cond"), P("val", "cond", None), P(None, "val"))
    body = make_body(mesh)

    return jax.shard_map(body, mesh=mesh, in_specs=placed, out_specs=P("val", "cond"), check_vma=False)
```

```python
import jax
import jax.numpy as jnp
from jax import lax
from jax.experimental import pallas as pl
from jax.experimental.pallas import tpu as pltpu
from jax.sharding import PartitionSpec as P


S = 64
CHUNKS = 4
GROUPS = 1

NT = (((1,), (1,)), ((), ()))
NN = (((1,), (0,)), ((), ()))


def group_size(count, rows):
    best = 1
    for size in range(1, count + 1):
        if count % size == 0 and size * rows <= 256:
            best = size
    return best


def chain(zed, entries, pc, accs):
    pieces, count, rows, depth = entries[0][0][0].shape
    total_g, cols, _ = pc.shape
    bands = entries[0][0][1].shape[2]
    many = len(entries[0])
    gg = group_size(total_g, rows * many)
    step_g = gg * GROUPS if total_g % (gg * GROUPS) == 0 else gg
    high = gg * many * rows
    first = [acc is None for acc in accs]

    def kernel(zed_ref, *refs):
        refs = list(refs)
        pc_ref = refs.pop(0)
        zed_at = zed_ref[0]
        t_refs = [[refs.pop(0) for _ in entry] for entry in entries]
        pv_refs = [[refs.pop(0) for _ in entry] for entry in entries]
        acc_refs = [None if f else refs.pop(0) for f in first]
        out_refs = [refs.pop(0) for _ in entries]
        token_ref, inner_ref = refs

        @pl.when(pl.program_id(0) == 0)
        def _():
            token_ref[...] = jnp.zeros(token_ref.shape, jnp.float32)
            for acc_ref, out_ref in zip(acc_refs, out_refs):
                if acc_ref is None:
                    out_ref[...] = jnp.zeros(out_ref.shape, jnp.float32)
                else:
                    out_ref[...] = acc_ref[...]

        for e in range(len(entries)):
            for base in range(0, step_g, gg):
                stacked = jnp.concatenate(
                    [pv_refs[e][u][base + g] for g in range(gg) for u in range(many)], axis=0)
                left = stacked.T
                for g in range(gg):
                    for u in range(many):
                        low = (g * many + u) * rows
                        inner = None
                        for d in range(pieces):
                            q = lax.rem(zed_at + (pieces - d), pieces)
                            if depth % 128:
                                weights = pc_ref[d, base + g]
                            else:
                                weights = pc_ref[base + g, :, d * depth:(d + 1) * depth]
                            part = lax.dot_general(
                                t_refs[e][u][q].reshape(count * rows, depth), weights, NT,
                                preferred_element_type=jnp.float32)
                            inner = part if inner is None else inner + part
                        inner_ref[e, :, low:low + rows, :] = inner.astype(jnp.bfloat16).reshape(count, rows, cols)
                for s in range(count):
                    out_refs[e][s] += lax.dot_general(left, inner_ref[e, s], NN, preferred_element_type=jnp.float32)

    def fixed(i, z):
        return (0, 0, 0)

    if depth % 128:
        pc = pc.reshape(total_g, cols, pieces, depth).transpose(2, 0, 1, 3)
        in_specs = [pl.BlockSpec((pieces, step_g, cols, depth), lambda i, z: (0, i, 0, 0))]
    else:
        in_specs = [pl.BlockSpec((step_g, cols, pieces * depth), lambda i, z: (i, 0, 0))]
    flat = [unit for entry in entries for unit in entry]
    in_specs += [pl.BlockSpec(
        (pieces, count, rows, depth), lambda i, z: (0, 0, 0, 0), pipeline_mode=pl.Buffered(1)) for _ in flat]
    in_specs += [pl.BlockSpec((step_g, rows, bands), lambda i, z: (i, 0, 0)) for _ in flat]
    operands = [pc] + [t for t, _ in flat] + [pv for _, pv in flat]
    aliases = {}
    for e, acc in enumerate(accs):
        if acc is not None:
            in_specs.append(pl.BlockSpec((count, bands, cols), fixed, pipeline_mode=pl.Buffered(1)))
            operands.append(acc)
            aliases[len(operands)] = e
    flops = 2 * len(flat) * count * total_g * rows * cols * (pieces * depth + bands)
    *outs, token = pl.pallas_call(
        kernel,
        out_shape=[jax.ShapeDtypeStruct((count, bands, cols), jnp.float32) for _ in entries]
        + [jax.ShapeDtypeStruct((8, 128), jnp.float32)],
        grid_spec=pltpu.PrefetchScalarGridSpec(
            num_scalar_prefetch=1,
            grid=(total_g // step_g,),
            in_specs=in_specs,
            out_specs=[pl.BlockSpec((count, bands, cols), fixed) for _ in entries]
            + [pl.BlockSpec((8, 128), lambda i, z: (0, 0))],
            scratch_shapes=[pltpu.VMEM((len(entries), count, high, cols), jnp.bfloat16)],
        ),
        input_output_aliases=aliases,
        compiler_params=pltpu.CompilerParams(
            dimension_semantics=("arbitrary",), vmem_limit_bytes=56 * 1024 * 1024),
        cost_estimate=pl.CostEstimate(
            flops=flops, transcendentals=0,
            bytes_accessed=total_g * cols * depth * pieces * 2 + len(entries) * count * bands * cols * 8),
        name="chain",
    )(zed, *operands)
    return outs, token


def after(value, *tokens):
    return lax.optimization_barrier((value, *tokens))[0]


def make_body(mesh):
    nv, nc = mesh.shape["val"], mesh.shape["cond"]
    nx = nv // 4

    def split(i):
        return i // (2 * nx), (i // 2) % nx, i % 2

    def join(y, x, k):
        return (y * nx + x) * 2 + k

    def flip_y(i):
        return lax.rem(i + 2 * nx, nv) if not isinstance(i, int) else (i + 2 * nx) % nv

    def send(value, table):
        return lax.ppermute(value, "val", table)

    to_twin = [(i, i ^ 1) for i in range(nv)]
    to_y = [(i, (i + 2 * nx) % nv) for i in range(nv)]

    def to_x(step):
        return [(i, join(split(i)[0], (split(i)[1] + step) % nx, split(i)[2])) for i in range(nv)]

    def to_z(step):
        return [(j, (j + step) % nc) for j in range(nc)]

    def body(trial, pair_cond, pair_val):
        me = lax.axis_index("val")
        zed = lax.axis_index("cond").astype(jnp.int32).reshape(1)
        core = lax.rem(me, 2)
        own_x = lax.rem(me // 2, nx)
        own_y = me // (2 * nx)
        wb = trial.shape[0]
        depth = trial.shape[1] // S
        bands = pair_val.shape[0]
        gb, cols, _ = pair_cond.shape
        vb = bands // nv
        half = S // 2
        n = half // CHUNKS

        pc_y = send(pair_cond, to_y)

        turned = trial.reshape(wb, depth, S).transpose(2, 0, 1)
        kept = lax.dynamic_slice_in_dim(turned, core * half, half, 0)
        given = lax.dynamic_slice_in_dim(turned, (1 - core) * half, half, 0)
        taken = send(given, to_twin)
        block = jnp.concatenate([kept, taken], axis=1)

        def around_z(part):
            return [part] + [lax.ppermute(part, "cond", to_z(q)) for q in range(1, nc)]

        parts = [around_z(block[:n])]

        flat = after(pair_val, block).T.reshape(wb, nv, gb, bands).transpose(1, 2, 0, 3)

        def blocks_for(dest):
            order = (dest, dest ^ 1, flip_y(dest), flip_y(dest) ^ 1)
            return jnp.stack([lax.dynamic_index_in_dim(flat, o, 0, keepdims=False) for o in order])

        def swap_pairs(a):
            return jnp.stack([a[1], a[0], a[3], a[2]])

        mine, twins = blocks_for(me), blocks_for(me ^ 1)
        far = []
        for step in range(1, nx):
            dest = (own_y * nx + lax.rem(own_x + step, nx)) * 2 + core
            far.append(blocks_for(dest))
        pv_near = jnp.concatenate([mine, send(twins, to_twin)], axis=2)
        far_got = [send(f, to_x(step)) for f, step in zip(far, range(1, nx))]
        pc_late = after(pair_cond, block)
        pc_own = jnp.concatenate([pc_late, send(pc_late, to_twin)], axis=0)
        for i in range(1, CHUNKS):
            parts.append(around_z(after(block[i * n:(i + 1) * n], *far)))

        def own_pv(pv):
            return pv[:2].reshape(2 * gb, 2 * wb, bands)

        accs = [None] * CHUNKS
        near, others = [None] * CHUNKS, [None] * CHUNKS
        token = None
        pv_all = [pv_near]
        for i in range(CHUNKS):
            got = list(lax.optimization_barrier((*parts[i], pc_own if token is None else token))[:-1])
            near[i] = jnp.stack(got)
            others[i] = [send(near[i], to_x(step)) for step in range(1, nx)]
            work = [(i, [(near[i], own_pv(pv_near))])]
            if i:
                for u in range(1, nx):
                    other = after(others[i - 1][u - 1], token)
                    work.append((i - 1, [(other, own_pv(pv_all[u]))]))
            for w in (work if nx > 2 else [work]):
                w = w if isinstance(w, list) else [w]
                outs, token = chain(zed, [e for _, e in w], pc_own, [accs[j] for j, _ in w])
                for (j, _), out in zip(w, outs):
                    accs[j] = out
            if i == 0:
                for got in far_got:
                    got = after(got, token)
                    pv_all.append(jnp.concatenate([got, send(swap_pairs(got), to_twin)], axis=2))
        pc_y = after(pc_y, token)
        pc_yt = send(pc_y, to_twin)

        def both(i, u, which):
            return [(t, pv[2 + which]) for t, pv in list(zip([near[i]] + others[i], pv_all))[u:u + 2]]

        def far_call(chunks, which, pc, token):
            for u in range(0, nx, 2):
                outs, token = chain(
                    zed, [both(i, u, which) for i in chunks], after(pc, token), [accs[i] for i in chunks])
                for i, out in zip(chunks, outs):
                    accs[i] = out
            return token

        last = CHUNKS - 1
        token = far_call([0, 1, 2, 3], 0, pc_y, token)
        for u in range(1, nx):
            (accs[last],), token = chain(
                zed, [[(after(others[last][u - 1], token), own_pv(pv_all[u]))]], pc_own, [accs[last]])

        def reduced(i):
            shaped = accs[i].reshape(n, 2, nx, 2 * vb, cols)

            def rows_of(y, x):
                block = lax.dynamic_slice(shaped, (0, y, x, 0, 0), (n, 1, 1, 2 * vb, cols))
                return block.reshape(n, 2 * vb, cols)

            total = rows_of(own_y, own_x)
            for dy in range(2):
                for dx in range(nx):
                    if dy or dx:
                        x = lax.rem(own_x + dx, nx)
                        y = own_y if dy == 0 else 1 - own_y
                        table = [
                            (j, join((split(j)[0] + dy) % 2, (split(j)[1] + dx) % nx, split(j)[2])) for j in range(nv)]
                        total = total + send(rows_of(y, x).astype(jnp.bfloat16), table).astype(jnp.float32)
            return total.astype(jnp.bfloat16)

        finals = []
        for chunks in ([0, 1], [2], [3]):
            token = far_call(chunks, 1, pc_yt, token)
            finals += [reduced(i) for i in chunks]
        done = jnp.concatenate(finals, axis=0).reshape(half, 2, vb, cols)
        mine = lax.dynamic_index_in_dim(done, core, 1, keepdims=False)
        other = send(lax.dynamic_index_in_dim(done, 1 - core, 1, keepdims=False), to_twin)
        low = jnp.where(core == 0, mine, other)
        high = jnp.where(core == 0, other, mine)
        whole = jnp.concatenate([low, high], axis=0)
        return whole.transpose(1, 2, 0).reshape(vb, cols * S)

    return body


def solution(mesh):
    placed = (P("val", "cond"), P("val", "cond", None), P(None, "val"))
    body = make_body(mesh)

    return jax.shard_map(body, mesh=mesh, in_specs=placed, out_specs=P("val", "cond"), check_vma=False)
```
